32 devices in a mesh: row: 8 (over y, x, core), col: 4 (over z).
Axes of the slice: x: 2, y: 2, z: 4, core: 2. Of those that a mesh axis runs over, the one named last changes fastest.
Arguments:
- features: bfloat16 [65536, 256], P(('col', 'row')), may hold values from -6 to 6
- block_values: bfloat16 [8, 4, 192, 128, 128], P('row', 'col'), may hold values from -0.1875 to 0.1875
- row_ptr: int32 [8, 4, 65], P('row', 'col'), may hold values from 0 to 144, as said below
- block_cols: int32 [8, 4, 192], P('row', 'col'), may hold values from 0 to 511, as said below
Outputs:
- product: bfloat16 [65536, 256], P(('row', 'col'))
The draws below stay inside these ranges and needn't reach their ends.
Inputs may be any that keep to these rules, and one draw needn't show every extreme that they name: row_ptr[r, c, 0] = 0, row_ptr never falls along its last dimension, row_ptr[r, c, 64] <= 144, and on exactly one device row_ptr[r, c, 64] = 144. block_cols[r, c, s] lies in c * 128 to (c + 1) * 128 - 1; a block column may repeat within a block row, and repeated blocks add.
All inputs are finite; a program needn't handle non-finite values.
Results may differ from the reference program's by a relative error of at most 0.001.
Values may be sent and summed in bfloat16 or wider, within the bound.
A program may use at most 128 MiB of HBM per device.

```python
import jax
import jax.numpy as jnp
from jax import lax

B = 128
NCOL = 256
BR = 64
SLOTS = 192
NB = 512
BC = 128
N_ROW = 8
N_COL = 4


def pattern(key):
    key_fill = jax.random.fold_in(key, 11)
    key_busy = jax.random.fold_in(key, 12)
    key_rows = jax.random.fold_in(key, 13)
    key_cols = jax.random.fold_in(key, 14)
    filled = SLOTS // 8 + jax.random.randint(key_fill, (N_ROW, N_COL), 0, SLOTS // 4 + 1)
    busiest = jax.random.randint(key_busy, (), 0, N_ROW * N_COL)
    position = jnp.arange(N_ROW * N_COL, dtype=jnp.int32).reshape(N_ROW, N_COL)
    filled = jnp.where(position == busiest, 3 * SLOTS // 4, filled)
    slot_ids = jnp.arange(SLOTS, dtype=jnp.int32)
    rows = jax.random.randint(key_rows, (N_ROW, N_COL, SLOTS), 0, BR)
    rows = jnp.where(slot_ids[None, None, :] < filled[:, :, None], rows, BR)
    bounds = jnp.arange(BR + 1, dtype=jnp.int32)
    pointers = jnp.sum((rows[:, :, None, :] < bounds[None, None, :, None]).astype(jnp.int32), axis=-1)
    group_start = (jnp.arange(N_COL, dtype=jnp.int32) * BC)[None, :, None]
    columns = jax.random.randint(key_cols, (N_ROW, N_COL, SLOTS), 0, BC) + group_start
    return (pointers.astype(jnp.int32), columns.astype(jnp.int32))


def draw_row_ptr(key, part):
    pointers, columns = pattern(key)
    return pointers


def draw_block_cols(key, part):
    pointers, columns = pattern(key)
    return columns


def level_of(rng, shape, pieces, low, top_value):
    gain = 1.0
    for dim, shards_of in pieces:
        heights = jax.random.uniform(jax.random.fold_in(jax.random.fold_in(rng, 6), dim), (shards_of,), jnp.float32, low / len(pieces), top_value / len(pieces))
        gain = gain * jnp.repeat(jnp.exp(heights), shape[dim] // shards_of).reshape((-1,) + (1,) * (len(shape) - 1 - dim))
    return gain


def scatter_about(rng, dims, scale, most, split=(), kind=jnp.bfloat16):
    array = scale * jax.random.normal(rng, dims, jnp.float32)
    if split:
        array = array * level_of(rng, dims, split, -0.22, 0.18)
    return jnp.clip(array, -most, most).astype(kind)


def setup_inputs(seed: int = 0) -> dict:
    seeds = jax.random.split(jax.random.key(seed), 5)
    features = scatter_about(seeds[0], (NB * B, NCOL), 1.0, 6.0, ((0, 32),))
    block_values = scatter_about(seeds[1], (N_ROW, N_COL, SLOTS, B, B), (9 * B) ** -0.5, 0.1875, ((0, 8), (1, 4)))
    row_ptr = draw_row_ptr(jax.random.fold_in(seeds[4], 71), 0)
    block_cols = draw_block_cols(jax.random.fold_in(seeds[4], 71), 0)
    return dict(features=features, block_values=block_values, row_ptr=row_ptr, block_cols=block_cols)


def row_weights(pointers, slot_count):
    slot_ids = jnp.arange(slot_count, dtype=jnp.int32)
    inside = (pointers[:-1, None] <= slot_ids[None, :]) & (slot_ids[None, :] < pointers[1:, None])
    return inside.astype(jnp.float32)


def reference(features, block_values, row_ptr, block_cols):
    block_size = block_values.shape[-1]
    panel = features.reshape(-1, block_size, features.shape[1])

    def one_group(operands):
        values_row, pointers_row, columns_row = operands

        def add_device(running, device_ops):
            values, pointers, columns = device_ops
            blocks = panel[columns.astype(jnp.int32)].astype(jnp.float32)
            products = jnp.einsum("sij,sjk->sik", values.astype(jnp.float32), blocks, precision=lax.Precision.HIGHEST)
            weights = row_weights(pointers.astype(jnp.int32), values.shape[0])
            summed = jnp.einsum("rs,sik->rik", weights, products, precision=lax.Precision.HIGHEST)
            return running + summed, jnp.zeros((), jnp.float32)

        starting = jnp.zeros((row_ptr.shape[2] - 1, block_size, features.shape[1]), jnp.float32)
        running, unused = lax.scan(add_device, starting, (values_row, pointers_row, columns_row))
        return running

    groups = lax.map(one_group, (block_values, row_ptr, block_cols))
    return groups.reshape(features.shape[0], features.shape[1]).astype(jnp.bfloat16)
```

```python
import functools

import jax
import jax.numpy as jnp
from jax import lax
from jax.experimental import pallas as pl
from jax.experimental.pallas import tpu as pltpu
from jax.sharding import PartitionSpec as P

LANES = 128
TOP = 32767.0
RIGHT, LEFT = 0, 1


def column_chunks(columns):
    chunks = [(0, 32), (32, 32), (64, 64)]
    for first in range(LANES, columns, 64):
        chunks.append((first, 64))
    return chunks


def parts_of(width, shard):
    parts = {32: 2, 64: 4, 128: 4}[width]
    while shard % parts:
        parts //= 2
    return parts


def kernel(
    n_row, n_col, pieces,
    pointers, block_cols, features, values_hbm, out,
    stage, panels, values, keep, sums, rows, tops, send_q, recv_q, send_s, recv_s,
    local_sem, ag_send, ag_recv, pair_send, pair_recv, rs_send, rs_recv, sc_send, sc_recv,
):
    n_chips = n_row // 2
    own_blocks = features.shape[0]
    block = features.shape[1]
    square = n_chips == 4
    halves = 2 if square else 1
    half = own_blocks // halves
    chunks = len(panels)
    live = values.shape[0]
    shard = out.shape[0]
    tiles = features.shape[2] // LANES
    r, c = lax.axis_index("row"), lax.axis_index("col")
    chip, core = r // 2, r % 2
    first_block = c * (own_blocks * n_row)
    parts = [p.shape[1] for p in tops]
    depth = [p.shape[1] for p in panels]
    fold = [block // d for d in depth]

    def chip_to(o):
        if square:
            y, x = chip // 2, chip % 2
            return (1 - y if o >= 2 else y) * 2 + (1 - x if o % 2 else x)
        return (chip + o) % n_chips

    def chip_from(o):
        return chip_to(o) if square else (chip + n_chips - o) % n_chips

    partner = chip * 2 + 1 - core
    direct = (1, 2) if square else tuple(range(1, n_chips))

    def slot(k, row, h):
        return panels[k].at[pl.ds(row * own_blocks + h * half, half)]

    own = [
        pltpu.make_async_copy(
            features.at[:, :, pl.ds(t * LANES, LANES)], stage.at[t], local_sem.at[t]
        )
        for t in range(tiles)
    ]
    for copy in own:
        copy.start()
    fetch = pltpu.make_async_copy(
        values_hbm.at[0, 0, pl.ds(0, live)], values, local_sem.at[tiles]
    )
    fetch.start()

    barrier = pltpu.get_barrier_semaphore()

    def greet(**where):
        pl.semaphore_signal(
            barrier, inc=1, device_id=where, device_id_type=pl.DeviceIdType.MESH
        )

    for o in direct:
        greet(row=chip_to(o) * 2 + core)
    greet(row=partner)
    pl.when(c > 0)(lambda: greet(col=c - 1))
    pl.when(c < n_col - 1)(lambda: greet(col=c + 1))

    lane = lax.broadcasted_iota(jnp.int32, (1, LANES), 1)

    def pack_own(k):
        first, width = pieces[k]
        tile, offset = first // LANES, first % LANES
        d, f = depth[k], fold[k]

        def one(b, carry):
            packed = None
            for m in range(f):
                x = stage[tile, b, pl.ds(m * d, d), :].astype(jnp.float32)
                x = pltpu.roll(x, (m * width - offset) % LANES, 1)
                packed = x if m == 0 else jnp.where(lane >= m * width, x, packed)
            panels[k][r * own_blocks + b] = packed.astype(jnp.bfloat16)
            return carry

        lax.fori_loop(0, own_blocks, one, 0)

    def remote(src, dst, send, recv, **where):
        return pltpu.make_async_remote_copy(
            src_ref=src, dst_ref=dst, send_sem=send, recv_sem=recv,
            device_id=where, device_id_type=pl.DeviceIdType.MESH,
        )

    def piece(k, o, h, source, to):
        return remote(
            slot(k, source * 2 + core, h), slot(k, source * 2 + core, h),
            ag_send.at[k, o, h], ag_recv.at[k, o, h], row=to * 2 + core,
        )

    def across(k, o, h):
        return piece(k, o, h, chip, chip_to(o))

    def arriving(k, o, h):
        return piece(k, o, h, chip_from(o), chip_from(o))

    def relay(k, h):
        return piece(k, 3, h, chip_from(1 + h), chip_to(2 - h))

    def pair(k, o, h, whose):
        row = (chip_from(o) if o else chip) * 2 + whose
        return remote(
            slot(k, row, h), slot(k, row, h), pair_send.at[k, o, h], pair_recv.at[k, o, h],
            row=partner,
        )

    if square:
        order = ((1, 0), (2, 1), (1, 1), (2, 0))
    else:
        order = tuple((o, 0) for o in direct)

    def gather_start(k):
        for o, h in order:
            across(k, o, h).start()
        for h in range(halves):
            pair(k, 0, h, core).start()

    def gather_relay(k):
        for o, h in order:
            arriving(k, o, h).wait_recv()
            if square and (o, h) in ((1, 0), (2, 1)):
                relay(k, h).start()
            pair(k, o, h, core).start()

    def gather_finish(k):
        if square:
            for h in range(halves):
                arriving(k, 3, h).wait_recv()
                pair(k, 3, h, core).start()
        for o in range(n_chips):
            for h in range(halves):
                pair(k, o, h, 1 - core).wait_recv()

    unroll = 1
    for u in (2, 4, 8, 16):
        if live % u == 0:
            unroll = u

    def mark_rows():
        ids = lax.broadcasted_iota(jnp.int32, keep.shape, 0)

        def mark(q, flags):
            return jnp.where(ids == pointers[0, 0, q], 0.0, flags)

        keep[...] = lax.fori_loop(0, pointers.shape[2], mark, jnp.ones(keep.shape, jnp.float32))

    def compute(k):
        width = pieces[k][1]

        def panel(s):
            x = panels[k][jnp.maximum(block_cols[0, 0, s] - first_block, 0)]
            if fold[k] == 1:
                return x
            turned = [x] + [pltpu.roll(x, LANES - m * width, 1) for m in range(1, fold[k])]
            return jnp.concatenate(turned, axis=0)

        def step(i, total):
            first = i * unroll
            products = [
                jnp.dot(values[first + u], panel(first + u), preferred_element_type=jnp.float32)
                for u in range(unroll)
            ]
            for u in range(unroll):
                total = total * keep[pl.ds(first + u, 1), :] + products[u]
                sums[first + u] = total
            return total

        lax.fori_loop(0, live // unroll, step, jnp.zeros(sums.shape[1:], jnp.float32))

    def row_sum(k, q):
        width, d = pieces[k][1], depth[k]
        begin, end = pointers[0, 0, q], pointers[0, 0, q + 1]
        last = jnp.maximum(end - 1, 0)
        packed = None
        for m in range(fold[k]):
            x = sums[last, pl.ds(m * d, d), :]
            if m == 0:
                packed = x
            else:
                packed = jnp.where(lane >= m * width, pltpu.roll(x, m * width, 1), packed)
        return packed * jnp.where(end > begin, 1.0, 0.0)

    def collect(k, j, s):
        width = shard // parts[k]

        def one(b, top):
            q = j * shard + s * width + b
            x = row_sum(k, q)
            rows[k][q] = x
            return jnp.maximum(top, jnp.max(jnp.abs(x).reshape(-1, 8, LANES), axis=0))

        top = lax.fori_loop(0, width, one, jnp.zeros((8, LANES), jnp.float32))
        tops[k][j, s] = jnp.max(top, axis=0, keepdims=True)

    def seat(way, j):
        return j + 1 if way == RIGHT else j

    def received(way, k, j, s, b):
        width = shard // parts[k]
        levels = recv_q[k][seat(way, j), s * width + b].astype(jnp.int32).astype(jnp.float32)
        return levels * recv_s[k][seat(way, j), s]

    def message(way, k, j, s):
        width = shard // parts[k]
        to = c + 1 if way == RIGHT else c - 1
        span = pl.ds(s * width, width)
        there = seat(way, j)
        return (
            remote(send_q[k].at[j, span], recv_q[k].at[there, span],
                   rs_send[k].at[j, s], rs_recv[k].at[there, s], col=to),
            remote(send_s[k].at[j, s], recv_s[k].at[there, s],
                   sc_send[k].at[j, s], sc_recv[k].at[there, s], col=to),
        )

    def forward(way, k, j, s, incoming):
        width = shard // parts[k]
        most = tops[k][j, s]
        if incoming:
            for copy in message(way, k, j, s):
                copy.wait_recv()
            most = most + recv_s[k][seat(way, j), s] * TOP
        most = jnp.maximum(most, 1e-30)
        send_s[k][j, s] = most * (1.0 / TOP)
        gain = TOP / most

        def one(b, carry):
            x = rows[k][j * shard + s * width + b]
            if incoming:
                x = x + received(way, k, j, s, b)
            send_q[k][j, s * width + b] = jnp.round(x * gain).astype(jnp.int32).astype(jnp.int16)
            return carry

        lax.fori_loop(0, width, one, 0)
        for copy in message(way, k, j, s):
            copy.start()

    def scatter_start(k):
        n = parts[k]

        def right(m, carry):
            collect(k, n_col - 1 - m // n, m % n)
            forward(RIGHT, k, n_col - 1 - m // n, m % n, False)
            return carry

        def left(m, carry):
            collect(k, m // n, m % n)
            forward(LEFT, k, m // n, m % n, False)
            return carry

        def keep_own(m, carry):
            collect(k, c, m)
            return carry

        def keep_all(m, carry):
            collect(k, m // n, m % n)
            return carry

        total = (n_col - 1) * n

        @pl.when(c == 0)
        def _():
            lax.fori_loop(0, total, right, 0)
            lax.fori_loop(0, n, keep_own, 0)

        @pl.when(c == n_col - 1)
        def _():
            lax.fori_loop(0, total, left, 0)
            lax.fori_loop(0, n, keep_own, 0)

        @pl.when((c > 0) & (c < n_col - 1))
        def _():
            lax.fori_loop(0, n_col * n, keep_all, 0)

    def scatter_middle(k):
        p = parts[k]

        def unit(n, carry):
            right = n - c
            left = n - (n_col - 1 - c)

            @pl.when((c > 0) & (right >= 0) & (right < (n_col - 1 - c) * p))
            def _():
                forward(RIGHT, k, n_col - 1 - right // p, right % p, True)

            @pl.when((c < n_col - 1) & (left >= 0) & (left < c * p))
            def _():
                forward(LEFT, k, left // p, left % p, True)

            return carry

        lax.fori_loop(1, (n_col - 2) * p + 1, unit, 0)

    def finish(k):
        first, columns = pieces[k]
        tile, offset = first // LANES, first % LANES
        width = shard // parts[k]
        d = depth[k]

        def write(ways):
            def part(s, carry):
                for way in ways:
                    for copy in message(way, k, c, s):
                        copy.wait_recv()

                def one(b, inner):
                    x = rows[k][c * shard + s * width + b]
                    for way in ways:
                        x = x + received(way, k, c, s, b)
                    for m in range(fold[k]):
                        y = pltpu.roll(x, (offset - m * columns) % LANES, 1)
                        out[s * width + b, pl.ds(m * d, d), pl.ds(first, columns)] = (
                            y[:, offset:offset + columns].astype(out.dtype)
                        )
                    return inner

                return lax.fori_loop(0, width, one, carry)

            lax.fori_loop(0, parts[k], part, 0)

        pl.when(c == 0)(lambda: write((LEFT,)))
        pl.when(c == n_col - 1)(lambda: write((RIGHT,)))
        pl.when((c > 0) & (c < n_col - 1))(lambda: write((RIGHT, LEFT)))

    own[0].wait()
    pack_own(0)
    ends = jnp.where(c > 0, 1, 0) + jnp.where(c < n_col - 1, 1, 0)
    pl.semaphore_wait(barrier, len(direct) + 1 + ends)
    gather_start(0)
    for copy in own[1:]:
        copy.wait()
    pack_own(1)
    mark_rows()
    gather_relay(0)
    gather_start(1)
    for k in range(2, chunks):
        pack_own(k)
    fetch.wait()
    gather_finish(0)
    for k in range(chunks):
        compute(k)
        scatter_start(k)
        if k + 1 < chunks:
            gather_relay(k + 1)
        if k + 2 < chunks:
            gather_start(k + 2)
        if k > 0:
            scatter_middle(k - 1)
            finish(k - 1)
        if k + 1 < chunks:
            gather_finish(k + 1)
    scatter_middle(chunks - 1)
    finish(chunks - 1)

    for k in range(chunks):
        for h in range(halves):
            for o in direct:
                across(k, o, h).wait_send()
            if square:
                relay(k, h).wait_send()
            for o in range(n_chips):
                pair(k, o, h, core).wait_send()
        for way in (RIGHT, LEFT):
            def drain(m, carry, way=way, k=k):
                j = m // parts[k]

                @pl.when((j > c) if way == RIGHT else (j < c))
                def _():
                    for copy in message(way, k, j, m % parts[k]):
                        copy.wait_send()

                return carry

            lax.fori_loop(0, n_col * parts[k], drain, 0)


def local(n_row, n_col, features, block_values, row_ptr, block_cols):
    slots, block = block_values.shape[2], block_values.shape[3]
    live = slots * 3 // 4
    own_blocks = features.shape[0] // block
    group_blocks = own_blocks * n_row
    columns = features.shape[1]
    pieces = column_chunks(columns)
    shard = (row_ptr.shape[2] - 1) // n_col
    parts = [parts_of(width, shard) for _, width in pieces]
    depth = [block * width // LANES for _, width in pieces]
    smem = pl.BlockSpec(memory_space=pltpu.SMEM)
    hbm = pl.BlockSpec(memory_space=pl.ANY)
    halves = 2 if n_row == 8 else 1
    gathers = (len(pieces), n_row // 2, halves)

    def per_chunk(make):
        return [make(p, d) for p, d in zip(parts, depth)]

    dma = pltpu.SemaphoreType.DMA
    result = pl.pallas_call(
        functools.partial(kernel, n_row, n_col, pieces),
        out_shape=jax.ShapeDtypeStruct((shard, block, columns), jnp.bfloat16),
        in_specs=[smem] * 2 + [hbm] * 2,
        out_specs=pl.BlockSpec(memory_space=pltpu.VMEM),
        scratch_shapes=[
            pltpu.VMEM((columns // LANES, own_blocks, block, LANES), jnp.bfloat16),
            per_chunk(lambda p, d: pltpu.VMEM((group_blocks, d, LANES), jnp.bfloat16)),
            pltpu.VMEM((live, block, block), jnp.bfloat16),
            pltpu.VMEM((live, LANES), jnp.float32),
            pltpu.VMEM((live, block, LANES), jnp.float32),
            per_chunk(lambda p, d: pltpu.VMEM((shard * n_col, d, LANES), jnp.float32)),
            per_chunk(lambda p, d: pltpu.VMEM((n_col, p, 1, LANES), jnp.float32)),
            per_chunk(lambda p, d: pltpu.VMEM((n_col, shard, d, LANES), jnp.int16)),
            per_chunk(lambda p, d: pltpu.VMEM((n_col + 1, shard, d, LANES), jnp.int16)),
            per_chunk(lambda p, d: pltpu.VMEM((n_col, p, 1, LANES), jnp.float32)),
            per_chunk(lambda p, d: pltpu.VMEM((n_col + 1, p, 1, LANES), jnp.float32)),
            dma((columns // LANES + 1,)),
        ]
        + [dma(gathers)] * 4
        + [
            per_chunk(lambda p, d: dma((n_col, p))),
            per_chunk(lambda p, d: dma((n_col + 1, p))),
            per_chunk(lambda p, d: dma((n_col, p))),
            per_chunk(lambda p, d: dma((n_col + 1, p))),
        ],
        compiler_params=pltpu.CompilerParams(
            collective_id=0, has_side_effects=True, vmem_limit_bytes=67043328
        ),
    )(row_ptr, block_cols, features.reshape(own_blocks, block, -1), block_values)
    return result.reshape(shard * block, -1)


def solution(mesh):
    return jax.shard_map(
        functools.partial(local, mesh.shape["row"], mesh.shape["col"]),
        mesh=mesh,
        in_specs=(
            P(("col", "row"), None),
            P("row", "col", None, None, None),
            P("row", "col", None),
            P("row", "col", None),
        ),
        out_specs=P(("row", "col"), None),
        check_vma=False,
    )
```

```python
import functools

import jax
import jax.numpy as jnp
from jax import lax
from jax.experimental import pallas as pl
from jax.experimental.pallas import tpu as pltpu
from jax.sharding import PartitionSpec as P

LANES = 128
TOP = 32767.0
RIGHT, LEFT = 0, 1


def column_chunks(columns):
    chunks = [(0, 32), (32, 32), (64, 64)]
    for first in range(LANES, columns, 64):
        chunks.append((first, 64))
    return chunks


def parts_of(width, shard):
    parts = {32: 1, 64: 2, 128: 4}[width]
    while shard % parts:
        parts //= 2
    return parts


def kernel(
    n_row, n_col, pieces,
    pointers_hbm, block_cols_hbm, features, values_hbm, out,
    pointers, block_cols, stage, panels, values, keep, sums, rows, tops, send_q, recv_q, send_s, recv_s,
    local_sem, table_sem, ag_send, ag_recv, pair_send, pair_recv, rs_send, rs_recv, sc_send, sc_recv,
):
    n_chips = n_row // 2
    own_blocks = features.shape[0]
    block = features.shape[1]
    square = n_chips == 4
    halves = 2 if square else 1
    half = own_blocks // halves
    chunks = len(panels)
    live = values.shape[0]
    shard = out.shape[0]
    tiles = features.shape[2] // LANES
    r, c = lax.axis_index("row"), lax.axis_index("col")
    chip, core = r // 2, r % 2
    first_block = c * (own_blocks * n_row)
    parts = [p.shape[1] for p in rs_recv]
    depth = [p.shape[1] for p in panels]
    fold = [block // d for d in depth]

    def chip_to(o):
        if square:
            y, x = chip // 2, chip % 2
            return (1 - y if o >= 2 else y) * 2 + (1 - x if o % 2 else x)
        return (chip + o) % n_chips

    def chip_from(o):
        return chip_to(o) if square else (chip + n_chips - o) % n_chips

    partner = chip * 2 + 1 - core
    direct = (1, 2) if square else tuple(range(1, n_chips))

    def slot(k, row, h):
        return panels[k].at[pl.ds(row * own_blocks + h * half, half)]

    own = [
        pltpu.make_async_copy(
            features.at[:, :, pl.ds(t * LANES, LANES)], stage.at[t], local_sem.at[t]
        )
        for t in range(tiles)
    ]
    for copy in own:
        copy.start()
    tables = [
        pltpu.make_async_copy(pointers_hbm, pointers, table_sem.at[0]),
        pltpu.make_async_copy(block_cols_hbm, block_cols, table_sem.at[1]),
    ]
    for copy in tables:
        copy.start()
    fetch = pltpu.make_async_copy(
        values_hbm.at[0, 0, pl.ds(0, live)], values, local_sem.at[tiles]
    )
    fetch.start()

    barrier = pltpu.get_barrier_semaphore()

    def greet(**where):
        pl.semaphore_signal(
            barrier, inc=1, device_id=where, device_id_type=pl.DeviceIdType.MESH
        )

    for o in direct:
        greet(row=chip_to(o) * 2 + core)
    greet(row=partner)
    pl.when(c > 0)(lambda: greet(col=c - 1))
    pl.when(c < n_col - 1)(lambda: greet(col=c + 1))

    lane = lax.broadcasted_iota(jnp.int32, (1, LANES), 1)

    def each(count, batch, body):
        while count % batch:
            batch //= 2

        def step(i, carry):
            body([i * batch + u for u in range(batch)])
            return carry

        lax.fori_loop(0, count // batch, step, 0)

    def pack_own(k):
        first, width = pieces[k]
        tile, offset = first // LANES, first % LANES
        d, f = depth[k], fold[k]

        def one(b):
            packed = None
            for m in range(f):
                x = stage[tile, b, pl.ds(m * d, d), :].astype(jnp.float32)
                x = pltpu.roll(x, (m * width - offset) % LANES, 1)
                packed = x if m == 0 else jnp.where(lane >= m * width, x, packed)
            return packed.astype(jnp.bfloat16)

        def some(blocks):
            for b, packed in [(b, one(b)) for b in blocks]:
                panels[k][r * own_blocks + b] = packed

        each(own_blocks, 4, some)

    def remote(src, dst, send, recv, **where):
        return pltpu.make_async_remote_copy(
            src_ref=src, dst_ref=dst, send_sem=send, recv_sem=recv,
            device_id=where, device_id_type=pl.DeviceIdType.MESH,
        )

    def piece(k, o, h, source, to):
        return remote(
            slot(k, source * 2 + core, h), slot(k, source * 2 + core, h),
            ag_send.at[k], ag_recv.at[k, o, h], row=to * 2 + core,
        )

    def across(k, o, h):
        return piece(k, o, h, chip, chip_to(o))

    def arriving(k, o, h):
        return piece(k, o, h, chip_from(o), chip_from(o))

    def relay(k, h):
        return piece(k, 3, h, chip_from(1 + h), chip_to(2 - h))

    def pair(k, o, h, whose):
        row = (chip_from(o) if o else chip) * 2 + whose
        return remote(
            slot(k, row, h), slot(k, row, h), pair_send.at[k], pair_recv.at[k], row=partner,
        )

    def gathered(k, count, sent):
        span = panels[k].at[pl.ds(0, count * own_blocks)]
        return remote(span, span, sent.at[k], pair_recv.at[k], row=partner)

    if square:
        order = ((1, 0), (2, 1), (1, 1), (2, 0))
    else:
        order = tuple((o, 0) for o in direct)

    def gather_start(k):
        for o, h in order:
            across(k, o, h).start()
        for h in range(halves):
            pair(k, 0, h, core).start()

    def gather_relay(k):
        for o, h in order:
            arriving(k, o, h).wait_recv()
            if square and (o, h) in ((1, 0), (2, 1)):
                relay(k, h).start()
            pair(k, o, h, core).start()

    def gather_finish(k):
        if square:
            for h in range(halves):
                arriving(k, 3, h).wait_recv()
                pair(k, 3, h, core).start()
        gathered(k, n_chips, pair_send).wait_recv()

    unroll = 1
    for u in (2, 4, 8, 16):
        if live % u == 0:
            unroll = u

    def mark_rows():
        ids = lax.broadcasted_iota(jnp.int32, keep.shape, 0)

        def mark(q, flags):
            return jnp.where(ids == pointers[0, 0, q], 0.0, flags)

        keep[...] = lax.fori_loop(0, pointers.shape[2], mark, jnp.ones(keep.shape, jnp.float32))

    def compute(k, between=None):
        width = pieces[k][1]

        def panel(s):
            x = panels[k][jnp.maximum(block_cols[0, 0, s] - first_block, 0)]
            if fold[k] == 1:
                return x
            turned = [x] + [pltpu.roll(x, LANES - m * width, 1) for m in range(1, fold[k])]
            return jnp.concatenate(turned, axis=0)

        def step(i, total):
            first = i * unroll
            products = [
                jnp.dot(values[first + u], panel(first + u), preferred_element_type=jnp.float32)
                for u in range(unroll)
            ]
            for u in range(unroll):
                total = total * keep[pl.ds(first + u, 1), :] + products[u]
                sums[first + u] = total
            return total

        steps = live // unroll
        total = jnp.zeros(sums.shape[1:], jnp.float32)
        if between is not None:
            total = lax.fori_loop(0, steps // 2, step, total)
            between()
            lax.fori_loop(steps // 2, steps, step, total)
        else:
            lax.fori_loop(0, steps, step, total)

    def row_sum(k, q):
        width, d = pieces[k][1], depth[k]
        begin, end = pointers[0, 0, q], pointers[0, 0, q + 1]
        last = jnp.maximum(end - 1, 0)
        packed = None
        for m in range(fold[k]):
            x = sums[last, pl.ds(m * d, d), :]
            if m == 0:
                packed = x
            else:
                packed = jnp.where(lane >= m * width, pltpu.roll(x, m * width, 1), packed)
        return packed * jnp.where(end > begin, 1.0, 0.0)

    def collect(k, j):
        width = shard // parts[k]

        def part(s, top):
            first = j * shard + s * width
            found = [row_sum(k, first + b) for b in range(width)]
            for b, x in enumerate(found):
                rows[k][first + b] = x
            for x in found:
                top = jnp.maximum(top, jnp.max(jnp.abs(x).reshape(-1, 8, LANES), axis=0))
            return top

        top = lax.fori_loop(0, parts[k], part, jnp.zeros((8, LANES), jnp.float32))
        tops[k][j] = jnp.max(top, axis=0, keepdims=True)

    def seat(way, j):
        return j + 1 if way == RIGHT else j

    def received(way, k, j, s, b):
        width = shard // parts[k]
        levels = recv_q[k][seat(way, j), s * width + b].astype(jnp.int32).astype(jnp.float32)
        return levels * recv_s[k][seat(way, j)]

    def message(way, k, j, s):
        width = shard // parts[k]
        span = pl.ds(s * width, width)
        there = seat(way, j)
        return remote(
            send_q[k].at[j, span], recv_q[k].at[there, span], rs_send.at[k], rs_recv[k].at[there, s],
            col=c + 1 if way == RIGHT else c - 1,
        )

    def scale(way, k, j):
        there = seat(way, j)
        return remote(
            send_s[k].at[j], recv_s[k].at[there], sc_send.at[k], sc_recv.at[k, there],
            col=c + 1 if way == RIGHT else c - 1,
        )

    def announce(way, k, j, incoming):
        most = tops[k][j]
        if incoming:
            scale(way, k, j).wait_recv()
            most = most + recv_s[k][seat(way, j)] * TOP
        send_s[k][j] = jnp.maximum(most, 1e-30) * (1.0 / TOP)
        scale(way, k, j).start()

    def forward(way, k, j, s, incoming):
        width = shard // parts[k]
        if incoming:
            message(way, k, j, s).wait_recv()
        gain = 1.0 / send_s[k][j]

        def one(b):
            x = rows[k][j * shard + s * width + b]
            if incoming:
                x = x + received(way, k, j, s, b)
            return jnp.round(x * gain).astype(jnp.int32).astype(jnp.int16)

        for b, levels in [(b, one(b)) for b in range(width)]:
            send_q[k][j, s * width + b] = levels
        message(way, k, j, s).start()

    def scatter_start(k):
        def ship(way, j):
            collect(k, j)
            announce(way, k, j, False)

            def part(s, carry):
                forward(way, k, j, s, False)
                return carry

            lax.fori_loop(0, parts[k], part, 0)

        def right(m, carry):
            ship(RIGHT, n_col - 1 - m)
            return carry

        def left(m, carry):
            ship(LEFT, m)
            return carry

        def keep_all(j, carry):
            collect(k, j)
            return carry

        @pl.when(c == 0)
        def _():
            lax.fori_loop(0, n_col - 1, right, 0)
            collect(k, c)

        @pl.when(c == n_col - 1)
        def _():
            lax.fori_loop(0, n_col - 1, left, 0)
            collect(k, c)

        @pl.when((c > 0) & (c < n_col - 1))
        def _():
            lax.fori_loop(0, n_col, keep_all, 0)

    def scatter_middle(k):
        p = parts[k]

        def unit(n, carry):
            right = n - c
            left = n - (n_col - 1 - c)

            def through(way, j, s):
                pl.when(s == 0)(lambda: announce(way, k, j, True))
                forward(way, k, j, s, True)

            @pl.when((c > 0) & (right >= 0) & (right < (n_col - 1 - c) * p))
            def _():
                through(RIGHT, n_col - 1 - right // p, right % p)

            @pl.when((c < n_col - 1) & (left >= 0) & (left < c * p))
            def _():
                through(LEFT, left // p, left % p)

            return carry

        lax.fori_loop(1, (n_col - 2) * p + 1, unit, 0)

    def finish(k):
        first, columns = pieces[k]
        tile, offset = first // LANES, first % LANES
        width = shard // parts[k]
        d = depth[k]

        def write(ways):
            for way in ways:
                scale(way, k, c).wait_recv()

            def part(s, carry):
                for way in ways:
                    message(way, k, c, s).wait_recv()

                def one(b):
                    x = rows[k][c * shard + s * width + b]
                    for way in ways:
                        x = x + received(way, k, c, s, b)
                    turned = [pltpu.roll(x, (offset - m * columns) % LANES, 1) for m in range(fold[k])]
                    return [y[:, offset:offset + columns].astype(out.dtype) for y in turned]

                for b, pieces_of in [(b, one(b)) for b in range(width)]:
                    for m, y in enumerate(pieces_of):
                        out[s * width + b, pl.ds(m * d, d), pl.ds(first, columns)] = y
                return carry

            lax.fori_loop(0, parts[k], part, 0)

        pl.when(c == 0)(lambda: write((LEFT,)))
        pl.when(c == n_col - 1)(lambda: write((RIGHT,)))
        pl.when((c > 0) & (c < n_col - 1))(lambda: write((RIGHT, LEFT)))

    own[0].wait()
    pack_own(0)
    for copy in tables:
        copy.wait()
    ends = jnp.where(c > 0, 1, 0) + jnp.where(c < n_col - 1, 1, 0)
    pl.semaphore_wait(barrier, len(direct) + 1 + ends)
    gather_start(0)
    for copy in own[1:]:
        copy.wait()
    pack_own(1)
    mark_rows()
    gather_relay(0)
    gather_start(1)
    for k in range(2, chunks):
        pack_own(k)
    fetch.wait()
    gather_finish(0)

    def advance(k):
        if k + 1 < chunks:
            gather_relay(k + 1)
        if k + 2 < chunks:
            gather_start(k + 2)

    for k in range(chunks):
        compute(k, (lambda: advance(0)) if k == 0 else None)
        scatter_start(k)
        if k > 0:
            advance(k)
        if k > 1:
            finish(k - 2)
        if k > 0:
            scatter_middle(k - 1)
        if k + 1 < chunks:
            gather_finish(k + 1)
    finish(chunks - 2)
    scatter_middle(chunks - 1)
    finish(chunks - 1)

    for k in range(chunks):
        gathered(k, n_chips - 1, ag_send).wait_send()
        gathered(k, n_chips, pair_send).wait_send()
        shards = pl.ds(0, n_col - 1)
        remote(send_q[k].at[shards], recv_q[k].at[shards], rs_send.at[k], rs_recv[k].at[0, 0],
               row=partner).wait_send()
        remote(send_s[k].at[shards], recv_s[k].at[shards], sc_send.at[k], sc_recv.at[k, 0],
               row=partner).wait_send()


def local(n_row, n_col, features, block_values, row_ptr, block_cols):
    slots, block = block_values.shape[2], block_values.shape[3]
    live = slots * 3 // 4
    own_blocks = features.shape[0] // block
    group_blocks = own_blocks * n_row
    columns = features.shape[1]
    pieces = column_chunks(columns)
    shard = (row_ptr.shape[2] - 1) // n_col
    parts = [parts_of(width, shard) for _, width in pieces]
    depth = [block * width // LANES for _, width in pieces]
    hbm = pl.BlockSpec(memory_space=pltpu.HBM)
    halves = 2 if n_row == 8 else 1
    gathers = (len(pieces), n_row // 2, halves)

    def per_chunk(make):
        return [make(p, d) for p, d in zip(parts, depth)]

    dma = pltpu.SemaphoreType.DMA
    result = pl.pallas_call(
        functools.partial(kernel, n_row, n_col, pieces),
        out_shape=jax.ShapeDtypeStruct((shard, block, columns), jnp.bfloat16),
        in_specs=[hbm] * 4,
        out_specs=pl.BlockSpec(memory_space=pltpu.VMEM),
        scratch_shapes=[
            pltpu.SMEM(row_ptr.shape, row_ptr.dtype),
            pltpu.SMEM(block_cols.shape, block_cols.dtype),
            pltpu.VMEM((columns // LANES, own_blocks, block, LANES), jnp.bfloat16),
            per_chunk(lambda p, d: pltpu.VMEM((group_blocks, d, LANES), jnp.bfloat16)),
            pltpu.VMEM((live, block, block), jnp.bfloat16),
            pltpu.VMEM((live, LANES), jnp.float32),
            pltpu.VMEM((live, block, LANES), jnp.float32),
            per_chunk(lambda p, d: pltpu.VMEM((shard * n_col, d, LANES), jnp.float32)),
            per_chunk(lambda p, d: pltpu.VMEM((n_col, 1, LANES), jnp.float32)),
            per_chunk(lambda p, d: pltpu.VMEM((n_col, shard, d, LANES), jnp.int16)),
            per_chunk(lambda p, d: pltpu.VMEM((n_col + 1, shard, d, LANES), jnp.int16)),
            per_chunk(lambda p, d: pltpu.VMEM((n_col, 1, LANES), jnp.float32)),
            per_chunk(lambda p, d: pltpu.VMEM((n_col + 1, 1, LANES), jnp.float32)),
            dma((columns // LANES + 1,)),
            dma((2,)),
            dma((len(pieces),)),
            dma(gathers),
            dma((len(pieces),)),
            dma((len(pieces),)),
            dma((len(pieces),)),
            per_chunk(lambda p, d: dma((n_col + 1, p))),
            dma((len(pieces),)),
            dma((len(pieces), n_col + 1)),
        ],
        compiler_params=pltpu.CompilerParams(
            collective_id=0, has_side_effects=True, vmem_limit_bytes=60000000
        ),
    )(row_ptr, block_cols, features.reshape(own_blocks, block, -1), block_values)
    return result.reshape(shard * block, -1)


def solution(mesh):
    return jax.shard_map(
        functools.partial(local, mesh.shape["row"], mesh.shape["col"]),
        mesh=mesh,
        in_specs=(
            P(("col", "row"), None),
            P("row", "col", None, None, None),
            P("row", "col", None),
            P("row", "col", None),
        ),
        out_specs=P(("row", "col"), None),
        check_vma=False,
    )
```

```python
import functools

import jax
import jax.numpy as jnp
from jax import lax
from jax.experimental import pallas as pl
from jax.experimental.pallas import tpu as pltpu
from jax.sharding import PartitionSpec as P

LANES = 128
TOP = 32767.0
RIGHT, LEFT = 0, 1


def column_chunks(columns):
    chunks = [(0, 32), (32, 32), (64, 64)]
    for first in range(LANES, columns, 64):
        chunks.append((first, 64))
    return chunks


def parts_of(width, shard):
    parts = {32: 1, 64: 2, 128: 4}[width]
    while shard % parts:
        parts //= 2
    return parts


def kernel(
    n_row, n_col, pieces,
    pointers_hbm, block_cols_hbm, features, values_hbm, out,
    pointers, block_cols, stage, panels, values, keep, sums, rows, tops, send_q, recv_q, send_s, recv_s,
    local_sem, table_sem, ag_send, ag_recv, pair_send, pair_recv, rs_send, rs_recv, sc_send, sc_recv,
):
    n_chips = n_row // 2
    own_blocks = features.shape[0]
    block = features.shape[1]
    square = n_chips == 4
    halves = 2 if square else 1
    half = own_blocks // halves
    chunks = len(panels)
    live = values.shape[0]
    shard = out.shape[0]
    tiles = features.shape[2] // LANES
    r, c = lax.axis_index("row"), lax.axis_index("col")
    chip, core = r // 2, r % 2
    first_block = c * (own_blocks * n_row)
    parts = [p.shape[1] for p in rs_recv]
    depth = [p.shape[1] for p in panels]
    fold = [block // d for d in depth]

    def chip_to(o):
        if square:
            y, x = chip // 2, chip % 2
            return (1 - y if o >= 2 else y) * 2 + (1 - x if o % 2 else x)
        return (chip + o) % n_chips

    def chip_from(o):
        return chip_to(o) if square else (chip + n_chips - o) % n_chips

    partner = chip * 2 + 1 - core
    direct = (1, 2) if square else tuple(range(1, n_chips))

    def slot(k, row, h):
        return panels[k].at[pl.ds(row * own_blocks + h * half, half)]

    own = [
        pltpu.make_async_copy(
            features.at[:, :, pl.ds(t * LANES, LANES)], stage.at[t], local_sem.at[t]
        )
        for t in range(tiles)
    ]
    for copy in own:
        copy.start()
    tables = [
        pltpu.make_async_copy(pointers_hbm, pointers, table_sem.at[0]),
        pltpu.make_async_copy(block_cols_hbm, block_cols, table_sem.at[1]),
    ]
    for copy in tables:
        copy.start()
    fetch = pltpu.make_async_copy(
        values_hbm.at[0, 0, pl.ds(0, live)], values, local_sem.at[tiles]
    )
    fetch.start()

    barrier = pltpu.get_barrier_semaphore()

    def greet(**where):
        pl.semaphore_signal(
            barrier, inc=1, device_id=where, device_id_type=pl.DeviceIdType.MESH
        )

    for o in direct:
        greet(row=chip_to(o) * 2 + core)
    greet(row=partner)
    pl.when(c > 0)(lambda: greet(col=c - 1))
    pl.when(c < n_col - 1)(lambda: greet(col=c + 1))

    lane = lax.broadcasted_iota(jnp.int32, (1, LANES), 1)

    def each(count, batch, body):
        while count % batch:
            batch //= 2

        def step(i, carry):
            body([i * batch + u for u in range(batch)])
            return carry

        lax.fori_loop(0, count // batch, step, 0)

    def pack_own(k):
        first, width = pieces[k]
        tile, offset = first // LANES, first % LANES
        d, f = depth[k], fold[k]

        def one(b):
            packed = None
            for m in range(f):
                x = stage[tile, b, pl.ds(m * d, d), :].astype(jnp.float32)
                x = pltpu.roll(x, (m * width - offset) % LANES, 1)
                packed = x if m == 0 else jnp.where(lane >= m * width, x, packed)
            return packed.astype(jnp.bfloat16)

        def some(blocks):
            for b, packed in [(b, one(b)) for b in blocks]:
                panels[k][r * own_blocks + b] = packed

        each(own_blocks, 4, some)

    def remote(src, dst, send, recv, **where):
        return pltpu.make_async_remote_copy(
            src_ref=src, dst_ref=dst, send_sem=send, recv_sem=recv,
            device_id=where, device_id_type=pl.DeviceIdType.MESH,
        )

    def piece(k, o, h, source, to):
        return remote(
            slot(k, source * 2 + core, h), slot(k, source * 2 + core, h),
            ag_send.at[k], ag_recv.at[k, o, h], row=to * 2 + core,
        )

    def across(k, o, h):
        return piece(k, o, h, chip, chip_to(o))

    def arriving(k, o, h):
        return piece(k, o, h, chip_from(o), chip_from(o))

    def relay(k, h):
        return piece(k, 3, h, chip_from(1 + h), chip_to(2 - h))

    def pair(k, o, h, whose):
        row = (chip_from(o) if o else chip) * 2 + whose
        return remote(
            slot(k, row, h), slot(k, row, h), pair_send.at[k], pair_recv.at[k], row=partner,
        )

    def gathered(k, count, sent):
        span = panels[k].at[pl.ds(0, count * own_blocks)]
        return remote(span, span, sent.at[k], pair_recv.at[k], row=partner)

    if square:
        order = ((1, 0), (2, 1), (1, 1), (2, 0))
    else:
        order = tuple((o, 0) for o in direct)

    def gather_start(k):
        for o, h in order:
            across(k, o, h).start()
        for h in range(halves):
            pair(k, 0, h, core).start()

    def gather_relay(k):
        for o, h in order:
            arriving(k, o, h).wait_recv()
            if square and (o, h) in ((1, 0), (2, 1)):
                relay(k, h).start()
            pair(k, o, h, core).start()

    def gather_finish(k):
        if square:
            for h in range(halves):
                arriving(k, 3, h).wait_recv()
                pair(k, 3, h, core).start()
        gathered(k, n_chips, pair_send).wait_recv()

    unroll = 1
    for u in (2, 4, 8, 16):
        if live % u == 0:
            unroll = u

    def mark_rows():
        ids = lax.broadcasted_iota(jnp.int32, keep.shape, 0)

        def mark(q, flags):
            return jnp.where(ids == pointers[0, 0, q], 0.0, flags)

        keep[...] = lax.fori_loop(0, pointers.shape[2], mark, jnp.ones(keep.shape, jnp.float32))

    def compute(k, between=None):
        width = pieces[k][1]

        def panel(s):
            x = panels[k][jnp.maximum(block_cols[0, 0, s] - first_block, 0)]
            if fold[k] == 1:
                return x
            turned = [x] + [pltpu.roll(x, LANES - m * width, 1) for m in range(1, fold[k])]
            return jnp.concatenate(turned, axis=0)

        def step(i, total):
            first = i * unroll
            products = [
                jnp.dot(values[first + u], panel(first + u), preferred_element_type=jnp.float32)
                for u in range(unroll)
            ]
            for u in range(unroll):
                total = total * keep[pl.ds(first + u, 1), :] + products[u]
                sums[first + u] = total
            return total

        steps = live // unroll
        total = jnp.zeros(sums.shape[1:], jnp.float32)
        if between is not None:
            total = lax.fori_loop(0, steps // 2, step, total)
            between()
            lax.fori_loop(steps // 2, steps, step, total)
        else:
            lax.fori_loop(0, steps, step, total)

    def row_sum(k, q):
        width, d = pieces[k][1], depth[k]
        begin, end = pointers[0, 0, q], pointers[0, 0, q + 1]
        last = jnp.maximum(end - 1, 0)
        packed = None
        for m in range(fold[k]):
            x = sums[last, pl.ds(m * d, d), :]
            if m == 0:
                packed = x
            else:
                packed = jnp.where(lane >= m * width, pltpu.roll(x, m * width, 1), packed)
        return packed * jnp.where(end > begin, 1.0, 0.0)

    def collect(k, j):
        width = shard // parts[k]

        def part(s, top):
            first = j * shard + s * width
            found = [row_sum(k, first + b) for b in range(width)]
            for b, x in enumerate(found):
                rows[k][first + b] = x
            for x in found:
                top = jnp.maximum(top, jnp.max(jnp.abs(x).reshape(-1, 8, LANES), axis=0))
            return top

        top = lax.fori_loop(0, parts[k], part, jnp.zeros((8, LANES), jnp.float32))
        tops[k][j] = jnp.max(top, axis=0, keepdims=True)

    def seat(way, j):
        return j + 1 if way == RIGHT else j

    def received(way, k, j, s, b):
        width = shard // parts[k]
        levels = recv_q[k][seat(way, j), s * width + b].astype(jnp.int32).astype(jnp.float32)
        return levels * recv_s[k][seat(way, j)]

    def message(way, k, j, s):
        width = shard // parts[k]
        span = pl.ds(s * width, width)
        there = seat(way, j)
        return remote(
            send_q[k].at[j, span], recv_q[k].at[there, span], rs_send.at[k], rs_recv[k].at[there, s],
            col=c + 1 if way == RIGHT else c - 1,
        )

    def scale(way, k, j):
        there = seat(way, j)
        return remote(
            send_s[k].at[j], recv_s[k].at[there], sc_send.at[k], sc_recv.at[k, there],
            col=c + 1 if way == RIGHT else c - 1,
        )

    def announce(way, k, j, incoming):
        most = tops[k][j]
        if incoming:
            scale(way, k, j).wait_recv()
            most = most + recv_s[k][seat(way, j)] * TOP
        send_s[k][j] = jnp.maximum(most, 1e-30) * (1.0 / TOP)
        scale(way, k, j).start()

    def forward(way, k, j, s, incoming):
        width = shard // parts[k]
        if incoming:
            message(way, k, j, s).wait_recv()
        gain = 1.0 / send_s[k][j]

        def one(b):
            x = rows[k][j * shard + s * width + b]
            if incoming:
                x = x + received(way, k, j, s, b)
            return jnp.round(x * gain).astype(jnp.int32).astype(jnp.int16)

        for b, levels in [(b, one(b)) for b in range(width)]:
            send_q[k][j, s * width + b] = levels
        message(way, k, j, s).start()

    def scatter_start(k):
        def ship(way, j):
            collect(k, j)
            announce(way, k, j, False)

            def part(s, carry):
                forward(way, k, j, s, False)
                return carry

            lax.fori_loop(0, parts[k], part, 0)

        def right(m, carry):
            ship(RIGHT, n_col - 1 - m)
            return carry

        def left(m, carry):
            ship(LEFT, m)
            return carry

        def keep_all(j, carry):
            collect(k, j)
            return carry

        @pl.when(c == 0)
        def _():
            lax.fori_loop(0, n_col - 1, right, 0)
            collect(k, c)

        @pl.when(c == n_col - 1)
        def _():
            lax.fori_loop(0, n_col - 1, left, 0)
            collect(k, c)

        @pl.when((c > 0) & (c < n_col - 1))
        def _():
            lax.fori_loop(0, n_col, keep_all, 0)

    def scatter_middle(k):
        p = parts[k]

        def unit(n, carry):
            right = n - c
            left = n - (n_col - 1 - c)

            def through(way, j, s):
                pl.when(s == 0)(lambda: announce(way, k, j, True))
                forward(way, k, j, s, True)

            @pl.when((c > 0) & (right >= 0) & (right < (n_col - 1 - c) * p))
            def _():
                through(RIGHT, n_col - 1 - right // p, right % p)

            @pl.when((c < n_col - 1) & (left >= 0) & (left < c * p))
            def _():
                through(LEFT, left // p, left % p)

            return carry

        lax.fori_loop(1, (n_col - 2) * p + 1, unit, 0)

    def scatter_hop(k, hop):
        p = parts[k]

        def through(way, j, s):
            pl.when(s == 0)(lambda: announce(way, k, j, True))
            forward(way, k, j, s, True)

        def right(m, carry):
            through(RIGHT, n_col - 1 - m // p, m % p)
            return carry

        def left(m, carry):
            through(LEFT, m // p, m % p)
            return carry

        total = (n_col - 1 - hop) * p

        @pl.when(c == hop)
        def _():
            lax.fori_loop(0, total, right, 0)

        @pl.when(n_col - 1 - c == hop)
        def _():
            lax.fori_loop(0, total, left, 0)

    def finish(k):
        first, columns = pieces[k]
        tile, offset = first // LANES, first % LANES
        width = shard // parts[k]
        d = depth[k]

        def write(ways):
            for way in ways:
                scale(way, k, c).wait_recv()

            def part(s, carry):
                for way in ways:
                    message(way, k, c, s).wait_recv()

                def one(b):
                    x = rows[k][c * shard + s * width + b]
                    for way in ways:
                        x = x + received(way, k, c, s, b)
                    turned = [pltpu.roll(x, (offset - m * columns) % LANES, 1) for m in range(fold[k])]
                    return [y[:, offset:offset + columns].astype(out.dtype) for y in turned]

                for b, pieces_of in [(b, one(b)) for b in range(width)]:
                    for m, y in enumerate(pieces_of):
                        out[s * width + b, pl.ds(m * d, d), pl.ds(first, columns)] = y
                return carry

            lax.fori_loop(0, parts[k], part, 0)

        pl.when(c == 0)(lambda: write((LEFT,)))
        pl.when(c == n_col - 1)(lambda: write((RIGHT,)))
        pl.when((c > 0) & (c < n_col - 1))(lambda: write((RIGHT, LEFT)))

    own[0].wait()
    pack_own(0)
    for copy in tables:
        copy.wait()
    ends = jnp.where(c > 0, 1, 0) + jnp.where(c < n_col - 1, 1, 0)
    pl.semaphore_wait(barrier, len(direct) + 1 + ends)
    gather_start(0)
    for copy in own[1:]:
        copy.wait()
    pack_own(1)
    mark_rows()
    gather_relay(0)
    gather_start(1)
    for k in range(2, chunks):
        pack_own(k)
    fetch.wait()
    gather_finish(0)

    def scatter_on(k):
        for hop in range(1, n_col - 1):
            if 0 <= k - hop < chunks - 1:
                scatter_hop(k - hop, hop)
        if 0 <= k - (n_col - 1) < chunks - 1:
            finish(k - (n_col - 1))

    def advance(k):
        if k + 1 < chunks:
            gather_relay(k + 1)
        if k + 2 < chunks:
            gather_start(k + 2)

    for k in range(chunks):
        compute(k, (lambda: advance(0)) if k == 0 else None)
        scatter_start(k)
        if k > 0:
            advance(k)
        scatter_on(k)
        if k + 1 < chunks:
            gather_finish(k + 1)
    for k in range(chunks, chunks + n_col - 2):
        scatter_on(k)
    scatter_middle(chunks - 1)
    finish(chunks - 1)

    for k in range(chunks):
        gathered(k, n_chips - 1, ag_send).wait_send()
        gathered(k, n_chips, pair_send).wait_send()
        shards = pl.ds(0, n_col - 1)
        remote(send_q[k].at[shards], recv_q[k].at[shards], rs_send.at[k], rs_recv[k].at[0, 0],
               row=partner).wait_send()
        remote(send_s[k].at[shards], recv_s[k].at[shards], sc_send.at[k], sc_recv.at[k, 0],
               row=partner).wait_send()


def local(n_row, n_col, features, block_values, row_ptr, block_cols):
    slots, block = block_values.shape[2], block_values.shape[3]
    live = slots * 3 // 4
    own_blocks = features.shape[0] // block
    group_blocks = own_blocks * n_row
    columns = features.shape[1]
    pieces = column_chunks(columns)
    shard = (row_ptr.shape[2] - 1) // n_col
    parts = [parts_of(width, shard) for _, width in pieces]
    depth = [block * width // LANES for _, width in pieces]
    hbm = pl.BlockSpec(memory_space=pltpu.HBM)
    halves = 2 if n_row == 8 else 1
    gathers = (len(pieces), n_row // 2, halves)

    def per_chunk(make):
        return [make(p, d) for p, d in zip(parts, depth)]

    dma = pltpu.SemaphoreType.DMA
    result = pl.pallas_call(
        functools.partial(kernel, n_row, n_col, pieces),
        out_shape=jax.ShapeDtypeStruct((shard, block, columns), jnp.bfloat16),
        in_specs=[hbm] * 4,
        out_specs=pl.BlockSpec(memory_space=pltpu.VMEM),
        scratch_shapes=[
            pltpu.SMEM(row_ptr.shape, row_ptr.dtype),
            pltpu.SMEM(block_cols.shape, block_cols.dtype),
            pltpu.VMEM((columns // LANES, own_blocks, block, LANES), jnp.bfloat16),
            per_chunk(lambda p, d: pltpu.VMEM((group_blocks, d, LANES), jnp.bfloat16)),
            pltpu.VMEM((live, block, block), jnp.bfloat16),
            pltpu.VMEM((live, LANES), jnp.float32),
            pltpu.VMEM((live, block, LANES), jnp.float32),
            per_chunk(lambda p, d: pltpu.VMEM((shard * n_col, d, LANES), jnp.float32)),
            per_chunk(lambda p, d: pltpu.VMEM((n_col, 1, LANES), jnp.float32)),
            per_chunk(lambda p, d: pltpu.VMEM((n_col, shard, d, LANES), jnp.int16)),
            per_chunk(lambda p, d: pltpu.VMEM((n_col + 1, shard, d, LANES), jnp.int16)),
            per_chunk(lambda p, d: pltpu.VMEM((n_col, 1, LANES), jnp.float32)),
            per_chunk(lambda p, d: pltpu.VMEM((n_col + 1, 1, LANES), jnp.float32)),
            dma((columns // LANES + 1,)),
            dma((2,)),
            dma((len(pieces),)),
            dma(gathers),
            dma((len(pieces),)),
            dma((len(pieces),)),
            dma((len(pieces),)),
            per_chunk(lambda p, d: dma((n_col + 1, p))),
            dma((len(pieces),)),
            dma((len(pieces), n_col + 1)),
        ],
        compiler_params=pltpu.CompilerParams(
            collective_id=0, has_side_effects=True, vmem_limit_bytes=50000000
        ),
    )(*[
        pltpu.with_memory_space_constraint(x, pltpu.HBM)
        for x in (row_ptr, block_cols, features.reshape(own_blocks, block, -1), block_values)
    ])
    return result.reshape(shard * block, -1)


def solution(mesh):
    return jax.shard_map(
        functools.partial(local, mesh.shape["row"], mesh.shape["col"]),
        mesh=mesh,
        in_specs=(
            P(("col", "row"), None),
            P("row", "col", None, None, None),
            P("row", "col", None),
            P("row", "col", None),
        ),
        out_specs=P(("row", "col"), None),
        check_vma=False,
    )
```

```python
import functools

import jax
import jax.numpy as jnp
from jax import lax
from jax.experimental import pallas as pl
from jax.experimental.pallas import tpu as pltpu
from jax.sharding import PartitionSpec as P

LANES = 128
TOP = 32767.0
RIGHT, LEFT = 0, 1


def column_chunks(columns):
    chunks = [(0, 32), (32, 32), (64, 64)]
    for first in range(LANES, columns, 64):
        chunks.append((first, 64))
    return chunks


def parts_of(width, shard):
    parts = {32: 1, 64: 2, 128: 4}[width]
    while shard % parts:
        parts //= 2
    return parts


def kernel(
    n_row, n_col, pieces,
    pointers_hbm, block_cols_hbm, features, values_hbm, out,
    pointers, block_cols, stage, panels, values, keep, sums, rows, tops, send_q, recv_q, send_s, recv_s,
    local_sem, table_sem, ag_send, ag_recv, pair_send, pair_recv, rs_send, rs_recv, sc_send, sc_recv,
):
    n_chips = n_row // 2
    own_blocks = features.shape[0]
    block = features.shape[1]
    square = n_chips == 4
    halves = 2 if square else 1
    half = own_blocks // halves
    chunks = len(panels)
    live = values.shape[0]
    shard = out.shape[0]
    tiles = features.shape[2] // LANES
    r, c = lax.axis_index("row"), lax.axis_index("col")
    chip, core = r // 2, r % 2
    first_block = c * (own_blocks * n_row)
    parts = [p.shape[1] for p in rs_recv]
    depth = [p.shape[1] for p in panels]
    fold = [block // d for d in depth]

    def chip_to(o):
        if square:
            y, x = chip // 2, chip % 2
            return (1 - y if o >= 2 else y) * 2 + (1 - x if o % 2 else x)
        return (chip + o) % n_chips

    def chip_from(o):
        return chip_to(o) if square else (chip + n_chips - o) % n_chips

    partner = chip * 2 + 1 - core
    others = (1, 2) if square else tuple(range(1, n_chips))

    def slot(k, row, h):
        return panels[k].at[pl.ds(row * own_blocks + h * half, half)]

    own = [
        pltpu.make_async_copy(
            features.at[:, :, pl.ds(t * LANES, LANES)], stage.at[t], local_sem.at[t]
        )
        for t in range(tiles)
    ]
    for copy in own:
        copy.start()
    tables = [
        pltpu.make_async_copy(pointers_hbm, pointers, table_sem.at[0]),
        pltpu.make_async_copy(block_cols_hbm, block_cols, table_sem.at[1]),
    ]
    for copy in tables:
        copy.start()
    fetch = pltpu.make_async_copy(
        values_hbm.at[0, 0, pl.ds(0, live)], values, local_sem.at[tiles]
    )
    fetch.start()

    barrier = pltpu.get_barrier_semaphore()

    def greet(**where):
        pl.semaphore_signal(
            barrier, inc=1, device_id=where, device_id_type=pl.DeviceIdType.MESH
        )

    for o in others:
        greet(row=chip_to(o) * 2 + core)
    greet(row=partner)
    pl.when(c > 0)(lambda: greet(col=c - 1))
    pl.when(c < n_col - 1)(lambda: greet(col=c + 1))

    lane = lax.broadcasted_iota(jnp.int32, (1, LANES), 1)

    def each(count, batch, body):
        while count % batch:
            batch //= 2

        def step(i, carry):
            body([i * batch + u for u in range(batch)])
            return carry

        lax.fori_loop(0, count // batch, step, 0)

    def pack_own(k):
        first, width = pieces[k]
        tile, offset = first // LANES, first % LANES
        d, f = depth[k], fold[k]

        def one(b):
            packed = None
            for m in range(f):
                x = stage[tile, b, pl.ds(m * d, d), :].astype(jnp.float32)
                x = pltpu.roll(x, (m * width - offset) % LANES, 1)
                packed = x if m == 0 else jnp.where(lane >= m * width, x, packed)
            return packed.astype(jnp.bfloat16)

        def some(blocks):
            for b, packed in [(b, one(b)) for b in blocks]:
                panels[k][r * own_blocks + b] = packed

        each(own_blocks, 4, some)

    def remote(src, dst, send, recv, **where):
        return pltpu.make_async_remote_copy(
            src_ref=src, dst_ref=dst, send_sem=send, recv_sem=recv,
            device_id=where, device_id_type=pl.DeviceIdType.MESH,
        )

    def piece(k, o, h, source, to):
        return remote(
            slot(k, source * 2 + core, h), slot(k, source * 2 + core, h),
            ag_send.at[k], ag_recv.at[k, o - 1, h], row=to * 2 + core,
        )

    def across(k, o, h):
        return piece(k, o, h, chip, chip_to(o))

    def arriving(k, o, h):
        return piece(k, o, h, chip_from(o), chip_from(o))

    def relay(k, h):
        return piece(k, 3, h, chip_from(1 + h), chip_to(2 - h))

    def pair(k, o, h, whose):
        row = (chip_from(o) if o else chip) * 2 + whose
        return remote(
            slot(k, row, h), slot(k, row, h), pair_send.at[k], pair_recv.at[k], row=partner,
        )

    def gathered(k, count, sent):
        span = panels[k].at[pl.ds(0, count * own_blocks)]
        return remote(span, span, sent.at[k], pair_recv.at[k], row=partner)

    if square:
        early, late = ((1, 0), (2, 1)), ((1, 1), (2, 0))
    else:
        early, late = tuple((o, 0) for o in others), ()

    def gather_early(k):
        for o, h in early:
            across(k, o, h).start()

    def gather_late(k):
        for o, h in late:
            across(k, o, h).start()
        for h in range(halves):
            pair(k, 0, h, core).start()

    def gather_relay(k):
        for o, h in early:
            arriving(k, o, h).wait_recv()
            if square:
                relay(k, h).start()
            pair(k, o, h, core).start()

    def gather_pass(k):
        for o, h in late:
            arriving(k, o, h).wait_recv()
            pair(k, o, h, core).start()

    def gather_finish(k):
        if square:
            for h in range(halves):
                arriving(k, 3, h).wait_recv()
                pair(k, 3, h, core).start()
        gathered(k, n_chips, pair_send).wait_recv()

    unroll = 1
    for u in (2, 4, 8, 16, 48):
        if live % u == 0:
            unroll = u

    def mark_rows():
        ids = lax.broadcasted_iota(jnp.int32, keep.shape, 0)

        def mark(q, flags):
            return jnp.where(ids == pointers[0, 0, q], 0.0, flags)

        keep[...] = lax.fori_loop(0, pointers.shape[2], mark, jnp.ones(keep.shape, jnp.float32))

    def compute(k, between=None):
        width = pieces[k][1]

        def panel(s):
            x = panels[k][jnp.maximum(block_cols[0, 0, s] - first_block, 0)]
            if fold[k] == 1:
                return x
            turned = [x] + [pltpu.roll(x, LANES - m * width, 1) for m in range(1, fold[k])]
            return jnp.concatenate(turned, axis=0)

        def step(i, total):
            first = i * unroll
            products = [
                jnp.dot(values[first + u], panel(first + u), preferred_element_type=jnp.float32)
                for u in range(unroll)
            ]
            for u in range(unroll):
                total = total * keep[pl.ds(first + u, 1), :] + products[u]
                sums[first + u] = total
            return total

        steps = live // unroll
        total = jnp.zeros(sums.shape[1:], jnp.float32)
        if between is not None:
            total = lax.fori_loop(0, steps // 2, step, total)
            between()
            lax.fori_loop(steps // 2, steps, step, total)
        else:
            lax.fori_loop(0, steps, step, total)

    def row_sum(k, q):
        width, d = pieces[k][1], depth[k]
        begin, end = pointers[0, 0, q], pointers[0, 0, q + 1]
        last = jnp.maximum(end - 1, 0)
        packed = None
        for m in range(fold[k]):
            x = sums[last, pl.ds(m * d, d), :]
            if m == 0:
                packed = x
            else:
                packed = jnp.where(lane >= m * width, pltpu.roll(x, m * width, 1), packed)
        return packed * jnp.where(end > begin, 1.0, 0.0)

    def collect(k, j):
        width = shard // parts[k]

        def part(s, top):
            first = j * shard + s * width
            found = [row_sum(k, first + b) for b in range(width)]
            for b, x in enumerate(found):
                rows[k][first + b] = x
            for x in found:
                top = jnp.maximum(top, jnp.max(jnp.abs(x).reshape(-1, 8, LANES), axis=0))
            return top

        top = lax.fori_loop(0, parts[k], part, jnp.zeros((8, LANES), jnp.float32))
        tops[k][j] = jnp.max(top, axis=0, keepdims=True)

    def seat(way, j):
        return j + 1 if way == RIGHT else j

    def received(way, k, j, s, b):
        width = shard // parts[k]
        levels = recv_q[k][seat(way, j), s * width + b].astype(jnp.int32).astype(jnp.float32)
        return levels * recv_s[k][seat(way, j)]

    def message(way, k, j, s):
        width = shard // parts[k]
        span = pl.ds(s * width, width)
        there = seat(way, j)
        return remote(
            send_q[k].at[j, span], recv_q[k].at[there, span], rs_send.at[k], rs_recv[k].at[there, s],
            col=c + 1 if way == RIGHT else c - 1,
        )

    def scale(way, k, j):
        there = seat(way, j)
        return remote(
            send_s[k].at[j], recv_s[k].at[there], sc_send.at[k], sc_recv.at[k, there],
            col=c + 1 if way == RIGHT else c - 1,
        )

    def announce(way, k, j, incoming):
        most = tops[k][j]
        if incoming:
            scale(way, k, j).wait_recv()
            most = most + recv_s[k][seat(way, j)] * TOP
        send_s[k][j] = jnp.maximum(most, 1e-30) * (1.0 / TOP)
        scale(way, k, j).start()

    def forward(way, k, j, s, incoming):
        width = shard // parts[k]
        if incoming:
            message(way, k, j, s).wait_recv()
        gain = 1.0 / send_s[k][j]

        def one(b):
            x = rows[k][j * shard + s * width + b]
            if incoming:
                x = x + received(way, k, j, s, b)
            return jnp.round(x * gain).astype(jnp.int32).astype(jnp.int16)

        for b, levels in [(b, one(b)) for b in range(width)]:
            send_q[k][j, s * width + b] = levels
        message(way, k, j, s).start()

    def scatter_start(k):
        def ship(way, j):
            collect(k, j)
            announce(way, k, j, False)

            def part(s, carry):
                forward(way, k, j, s, False)
                return carry

            lax.fori_loop(0, parts[k], part, 0)

        def right(m, carry):
            ship(RIGHT, n_col - 1 - m)
            return carry

        def left(m, carry):
            ship(LEFT, m)
            return carry

        def keep_all(j, carry):
            collect(k, j)
            return carry

        @pl.when(c == 0)
        def _():
            lax.fori_loop(0, n_col - 1, right, 0)
            collect(k, c)

        @pl.when(c == n_col - 1)
        def _():
            lax.fori_loop(0, n_col - 1, left, 0)
            collect(k, c)

        @pl.when((c > 0) & (c < n_col - 1))
        def _():
            lax.fori_loop(0, n_col, keep_all, 0)

    def scatter_middle(k):
        p = parts[k]

        def unit(n, carry):
            right = n - c
            left = n - (n_col - 1 - c)

            def through(way, j, s):
                pl.when(s == 0)(lambda: announce(way, k, j, True))
                forward(way, k, j, s, True)

            @pl.when((c > 0) & (right >= 0) & (right < (n_col - 1 - c) * p))
            def _():
                through(RIGHT, n_col - 1 - right // p, right % p)

            @pl.when((c < n_col - 1) & (left >= 0) & (left < c * p))
            def _():
                through(LEFT, left // p, left % p)

            return carry

        lax.fori_loop(1, (n_col - 2) * p + 1, unit, 0)

    def scatter_hop(k, hop):
        p = parts[k]

        def through(way, j, s):
            pl.when(s == 0)(lambda: announce(way, k, j, True))
            forward(way, k, j, s, True)

        def right(m, carry):
            through(RIGHT, n_col - 1 - m // p, m % p)
            return carry

        def left(m, carry):
            through(LEFT, m // p, m % p)
            return carry

        total = (n_col - 1 - hop) * p

        @pl.when(c == hop)
        def _():
            lax.fori_loop(0, total, right, 0)

        @pl.when(n_col - 1 - c == hop)
        def _():
            lax.fori_loop(0, total, left, 0)

    def finish(k):
        first, columns = pieces[k]
        tile, offset = first // LANES, first % LANES
        width = shard // parts[k]
        d = depth[k]

        def write(ways):
            for way in ways:
                scale(way, k, c).wait_recv()

            def part(s, carry):
                for way in ways:
                    message(way, k, c, s).wait_recv()

                def one(b):
                    x = rows[k][c * shard + s * width + b]
                    for way in ways:
                        x = x + received(way, k, c, s, b)
                    turned = [pltpu.roll(x, (offset - m * columns) % LANES, 1) for m in range(fold[k])]
                    return [y[:, offset:offset + columns].astype(out.dtype) for y in turned]

                for b, pieces_of in [(b, one(b)) for b in range(width)]:
                    for m, y in enumerate(pieces_of):
                        out[s * width + b, pl.ds(m * d, d), pl.ds(first, columns)] = y
                return carry

            lax.fori_loop(0, parts[k], part, 0)

        pl.when(c == 0)(lambda: write((LEFT,)))
        pl.when(c == n_col - 1)(lambda: write((RIGHT,)))
        pl.when((c > 0) & (c < n_col - 1))(lambda: write((RIGHT, LEFT)))

    own[0].wait()
    pack_own(0)
    for copy in tables:
        copy.wait()
    ends = jnp.where(c > 0, 1, 0) + jnp.where(c < n_col - 1, 1, 0)
    pl.semaphore_wait(barrier, len(others) + 1 + ends)
    gather_early(0)
    gather_late(0)
    for copy in own[1:]:
        copy.wait()
    pack_own(1)
    gather_early(1)
    gather_relay(0)
    gather_late(1)
    mark_rows()
    for k in range(2, chunks):
        pack_own(k)
    gather_pass(0)
    fetch.wait()
    gather_finish(0)

    def scatter_on(k):
        if 0 <= k - (n_col - 1) < chunks - 1:
            finish(k - (n_col - 1))
        for hop in range(n_col - 2, 0, -1):
            if 0 <= k - hop < chunks - 1:
                scatter_hop(k - hop, hop)

    def advance(k):
        if k + 1 < chunks:
            gather_relay(k + 1)
        if k + 2 < chunks:
            gather_early(k + 2)
            gather_late(k + 2)

    advance(0)
    for k in range(chunks):
        if k == 0:
            compute(k)
        else:
            compute(k, lambda: advance(k))
        scatter_start(k)
        if k < chunks - 1:
            gather_pass(k + 1)
        scatter_on(k)
        if k + 1 < chunks:
            gather_finish(k + 1)
    for k in range(chunks, chunks + n_col - 2):
        scatter_on(k)
    scatter_middle(chunks - 1)
    finish(chunks - 1)

    for k in range(chunks):
        gathered(k, n_chips - 1, ag_send).wait_send()
        gathered(k, n_chips, pair_send).wait_send()
        shards = pl.ds(0, n_col - 1)
        remote(send_q[k].at[shards], recv_q[k].at[shards], rs_send.at[k], rs_recv[k].at[0, 0],
               row=partner).wait_send()
        remote(send_s[k].at[shards], recv_s[k].at[shards], sc_send.at[k], sc_recv.at[k, 0],
               row=partner).wait_send()


def local(n_row, n_col, features, block_values, row_ptr, block_cols):
    slots, block = block_values.shape[2], block_values.shape[3]
    live = slots * 3 // 4
    own_blocks = features.shape[0] // block
    group_blocks = own_blocks * n_row
    columns = features.shape[1]
    pieces = column_chunks(columns)
    shard = (row_ptr.shape[2] - 1) // n_col
    parts = [parts_of(width, shard) for _, width in pieces]
    parts[-1] = parts_of(LANES, shard)
    depth = [block * width // LANES for _, width in pieces]
    hbm = pl.BlockSpec(memory_space=pltpu.HBM)
    halves = 2 if n_row == 8 else 1
    gathers = (len(pieces), max(n_row // 2 - 1, 1), halves)

    def per_chunk(make):
        return [make(p, d) for p, d in zip(parts, depth)]

    dma = pltpu.SemaphoreType.DMA
    result = pl.pallas_call(
        functools.partial(kernel, n_row, n_col, pieces),
        out_shape=jax.ShapeDtypeStruct((shard, block, columns), jnp.bfloat16),
        in_specs=[hbm] * 4,
        out_specs=pl.BlockSpec(memory_space=pltpu.VMEM),
        scratch_shapes=[
            pltpu.SMEM(row_ptr.shape, row_ptr.dtype),
            pltpu.SMEM(block_cols.shape, block_cols.dtype),
            pltpu.VMEM((columns // LANES, own_blocks, block, LANES), jnp.bfloat16),
            per_chunk(lambda p, d: pltpu.VMEM((group_blocks, d, LANES), jnp.bfloat16)),
            pltpu.VMEM((live, block, block), jnp.bfloat16),
            pltpu.VMEM((live, LANES), jnp.float32),
            pltpu.VMEM((live, block, LANES), jnp.float32),
            per_chunk(lambda p, d: pltpu.VMEM((shard * n_col, d, LANES), jnp.float32)),
            per_chunk(lambda p, d: pltpu.VMEM((n_col, 1, LANES), jnp.float32)),
            per_chunk(lambda p, d: pltpu.VMEM((n_col, shard, d, LANES), jnp.int16)),
            per_chunk(lambda p, d: pltpu.VMEM((n_col + 1, shard, d, LANES), jnp.int16)),
            per_chunk(lambda p, d: pltpu.VMEM((n_col, 1, LANES), jnp.float32)),
            per_chunk(lambda p, d: pltpu.VMEM((n_col + 1, 1, LANES), jnp.float32)),
            dma((columns // LANES + 1,)),
            dma((2,)),
            dma((len(pieces),)),
            dma(gathers),
            dma((len(pieces),)),
            dma((len(pieces),)),
            dma((len(pieces),)),
            per_chunk(lambda p, d: dma((n_col + 1, p))),
            dma((len(pieces),)),
            dma((len(pieces), n_col + 1)),
        ],
        compiler_params=pltpu.CompilerParams(
            collective_id=0, has_side_effects=True, vmem_limit_bytes=50000000
        ),
    )(*[
        pltpu.with_memory_space_constraint(x, pltpu.HBM)
        for x in (row_ptr, block_cols, features.reshape(own_blocks, block, -1), block_values)
    ])
    return result.reshape(shard * block, -1)


def solution(mesh):
    return jax.shard_map(
        functools.partial(local, mesh.shape["row"], mesh.shape["col"]),
        mesh=mesh,
        in_specs=(
            P(("col", "row"), None),
            P("row", "col", None, None, None),
            P("row", "col", None),
            P("row", "col", None),
        ),
        out_specs=P(("row", "col"), None),
        check_vma=False,
    )
```
